32 devices in a mesh: grp: 2 (over core), dev: 16 (over z, y, x).
Axes of the slice: x: 2, y: 2, z: 4, core: 2. Of those that a mesh axis runs over, the one named last changes fastest.
Arguments:
- pixel_tiles: float32 [2048, 6, 512], P(('grp', 'dev')), may hold values from -31 to 31
- blend_source: int32 [2048, 2], P(('grp', 'dev')), may hold values from 0 to 15, all different within a row; in each aligned block of 64 rows (0 to 63, 64 to 127, ...) at most 8 rows name the same one
- blend_slot: int32 [2048, 2], P(('grp', 'dev')), may hold values from 0 to 63
- component_count: int32 [2048], P(('grp', 'dev')), may hold values from 12 to 24
- sed_start: bfloat16 [2048, 24, 6], P(('grp', 'dev')), may hold values from 0.049804688 to 0.5
- morph_start: bfloat16 [2048, 2, 24, 512], P(('grp', 'dev')), may hold values from 0.019897461 to 0.5
Outputs:
- whitened: float32 [2048, 6, 512], P(('grp', 'dev'))
- sed_final: bfloat16 [2048, 24, 6], P(('grp', 'dev'))
The draws below stay inside these ranges and needn't reach their ends.
Inputs may be any that keep to these rules, and one draw needn't show every extreme that they name: `blend_source`: each blend names 2 different devices of its region; over the blends of one device no device is named more than 8 times, and some device is named exactly 8 times. `blend_slot`: several blends may name the same tile.
All inputs are finite; a program needn't handle non-finite values.
Results may differ from the reference program's by a relative error of at most 0.0052.
Values may be sent and summed in bfloat16 or wider, within the bound.
A program may use at most 64 MiB of HBM per device.

```python
import math
import jax
import jax.numpy as jnp
import numpy as np
from jax import lax

BANDS = 6
COMPONENTS = 24
PIX = 512
FOOT = 2
ITERS = 2
TILE_DEV = 64
BLEND_DEV = 64
CAPACITY = 8
TILES_G = 1024
BLENDS_G = 1024
TILES_ALL = 2048
BLENDS_ALL = 2048
N_DEV = 16


def draw_pixel_tiles(key, part):
    key_base, key_rough = jax.random.split(jax.random.fold_in(key, 11), 2)
    shape = (TILES_ALL, BANDS, PIX)
    position = (jnp.arange(TILES_ALL, dtype=jnp.int32) % TILES_G).astype(jnp.float32) / TILES_G
    rough = jnp.exp(jax.random.uniform(key_rough, (TILES_ALL, 1, 1), jnp.float32, -0.7, 0.7))
    scale = jnp.power(3.0, position)[:, None, None] * rough
    base = jnp.clip(jax.random.normal(key_base, shape, jnp.float32), -5.0, 5.0)
    return (base * scale).astype(jnp.float32)


def with_ends(drawn, stream_key, low, top_value):
    index_at = [jax.random.randint(jax.random.fold_in(stream_key, axis), (), 0, length) for axis, length in enumerate(drawn.shape)]
    widest = drawn.shape.index(max(drawn.shape))
    next_to = index_at[:widest] + [(index_at[widest] + 1) % drawn.shape[widest]] + index_at[widest + 1:]
    return drawn.at[tuple(index_at)].set(low).at[tuple(next_to)].set(top_value)


def levels(stream_key, extent, pieces, smallest, high):
    def one(axis_at, parts):
        heights = jax.random.uniform(jax.random.fold_in(jax.random.fold_in(stream_key, 6), axis_at), (parts,), jnp.float32, smallest / len(pieces), high / len(pieces))
        return jnp.repeat(jnp.exp(heights), extent[axis_at] // parts).reshape((-1,) + (1,) * (len(extent) - axis_at - 1))

    factor_of = one(*pieces[0])
    for cut in pieces[1:]:
        factor_of = factor_of * one(*cut)
    return factor_of


def shared_out(rng, own, number, rows, amount, top, most, skew):
    sequence = jax.random.permutation(rng, amount)
    packed, ordinary = load_shares(amount, rows * top, most, skew, True), load_shares(amount, rows * top, most, skew, False)
    places = jnp.arange(amount)

    def named(tallies, turn):
        used = int((tallies > 0).sum())
        fixed = max(1, used // 4)
        shifted = fixed + (places - fixed + turn * (used - fixed)) % max(1, amount - fixed)
        return jnp.zeros((amount,), jnp.int32).at[sequence[jnp.where(places < fixed, places, shifted)]].set(jnp.asarray(tallies, jnp.int32))

    tallies = jnp.where(number % 4 == 0, named(packed, number // 4), named(ordinary, number - number // 4 - 1))
    mixed = jax.random.permutation(jax.random.fold_in(own, 3), amount)
    donor, taker = mixed[0:amount // 2 * 2:2], mixed[1:amount // 2 * 2:2]
    slack = jnp.minimum(tallies[donor] - 1, most - tallies[taker]) // 2
    slack = jnp.where((donor == sequence[0]) | (taker == sequence[0]) | (tallies[taker] == 0), 0, jnp.maximum(slack, 0))
    shifted = jax.random.randint(jax.random.fold_in(own, 4), (amount // 2,), 0, 1 << 20) % (slack + 1)
    tallies = tallies.at[donor].add(-shifted).at[taker].add(shifted)
    labels = jnp.searchsorted(jnp.cumsum(tallies), jnp.arange(rows * top), side="right").astype(jnp.int32)
    listing = labels.reshape(top, rows).T
    listing = listing[jax.random.permutation(jax.random.fold_in(own, 1), rows)]
    turn = jax.random.randint(jax.random.fold_in(own, 2), (rows, 1), 0, top)
    return jnp.take_along_axis(listing, (jnp.arange(top)[None, :] + turn) % top, axis=1)


def load_shares(number_of, total, limit, skew, full):
    weights = [(1 << 20) // math.isqrt(grade ** skew) + 1 for grade in range(1, number_of + 1)]
    largest = limit if full else min(limit, max(-(-total // number_of), total * weights[0] // sum(weights)))
    least = 1 if total - largest >= number_of - 1 else 0
    counts, spare = [largest] + [least] * (number_of - 1), total - largest - least * (number_of - 1)
    while spare > 0:
        movable = [i for i in range(1, number_of) if counts[i] < largest] or [i for i in range(1, number_of) if counts[i] < limit]
        mass, left = sum([weights[i] for i in movable]), spare
        for i in movable:
            more = min(limit - counts[i], max(1, left * weights[i] // mass), spare)
            counts[i] = counts[i] + more
            spare = spare - more
    return np.array(counts)


def setup_inputs(seed: int = 0) -> dict:
    streams_of = jax.random.split(jax.random.key(seed), 7)
    pixel_tiles = draw_pixel_tiles(jax.random.fold_in(streams_of[6], 71), 0)
    blend_source_keys = jax.random.split(jax.random.fold_in(streams_of[1], 1), BLENDS_ALL // BLEND_DEV)
    blend_source_turns = jax.random.permutation(jax.random.fold_in(streams_of[1], 3), BLENDS_ALL // BLEND_DEV)
    blend_source = jax.vmap(lambda own, number: shared_out(jax.random.fold_in(streams_of[1], 2), own, number, BLEND_DEV, N_DEV, FOOT, CAPACITY, 2))(blend_source_keys, blend_source_turns).reshape((BLENDS_ALL, FOOT))
    blend_slot = with_ends(jax.random.randint(streams_of[2], (BLENDS_ALL, FOOT), 0, TILE_DEV), jax.random.fold_in(streams_of[2], 1), 0, TILE_DEV - 1).astype(jnp.int32)
    component_count = with_ends(jax.random.randint(streams_of[3], (BLENDS_ALL,), COMPONENTS // 2, COMPONENTS + 1), jax.random.fold_in(streams_of[3], 1), COMPONENTS // 2, COMPONENTS).astype(jnp.int32)
    sed_start = jnp.clip(jnp.exp(math.log(0.5) - 2.306499 * jax.random.uniform(streams_of[4], (BLENDS_ALL, COMPONENTS, BANDS), jnp.float32) ** levels(streams_of[4], (BLENDS_ALL, COMPONENTS, BANDS), ((0, 32),), -0.2, 0.2)), 0.049804688, 0.5).astype(jnp.bfloat16)
    morph_start = jnp.clip(jnp.exp(math.log(0.5) - 3.224016 * jax.random.uniform(streams_of[5], (BLENDS_ALL, FOOT, COMPONENTS, PIX), jnp.float32) ** levels(streams_of[5], (BLENDS_ALL, FOOT, COMPONENTS, PIX), ((0, 32),), -0.2, 0.2)), 0.019897461, 0.5).astype(jnp.bfloat16)
    return dict(pixel_tiles=pixel_tiles, blend_source=blend_source, blend_slot=blend_slot, component_count=component_count, sed_start=sed_start, morph_start=morph_start)


def to_bf16(values):
    return lax.optimization_barrier(values.astype(jnp.bfloat16)).astype(jnp.float32)

def fit_block(blend_data, sed, morph, count):
    active = (jnp.arange(COMPONENTS, dtype=jnp.int32)[None, :] < count[:, None]).astype(jnp.float32)
    sed = sed.astype(jnp.float32) * active[:, :, None]
    morph = morph.astype(jnp.float32) * active[:, None, :, None]
    target = blend_data.astype(jnp.float32)
    for sweep in range(ITERS):
        misfit = to_bf16(jnp.einsum('nkb,nfkp->nfbp', sed, morph) - target)
        gram_matrix = jnp.einsum('nfkp,nfjp->nkj', morph, morph)
        lip_sed = jnp.sqrt(lax.optimization_barrier(jnp.sum(gram_matrix * gram_matrix, axis=(1, 2)))) + 1.0
        gradient = jnp.einsum('nfkp,nfbp->nkb', morph, misfit)
        sed = to_bf16(jnp.maximum(sed - gradient / lip_sed[:, None, None], 0.0) * active[:, :, None])
        misfit = to_bf16(jnp.einsum('nkb,nfkp->nfbp', sed, morph) - target)
        sed_gram = jnp.einsum('nkb,nkc->nbc', sed, sed)
        lip_morph = jnp.sqrt(lax.optimization_barrier(jnp.sum(sed_gram * sed_gram, axis=(1, 2)))) + 1.0
        grad_morph = jnp.einsum('nkb,nfbp->nfkp', sed, misfit)
        morph = to_bf16(jnp.maximum(morph - (grad_morph + 0.1) / lip_morph[:, None, None, None], 0.0) * active[:, None, :, None])
    model_out = jnp.einsum('nkb,nfkp->nfbp', sed, morph).astype(jnp.bfloat16)
    return (sed.astype(jnp.bfloat16), model_out)

def reference(pixel_tiles, blend_source, blend_slot, component_count, sed_start, morph_start):
    group_of = jnp.arange(BLENDS_ALL, dtype=jnp.int32) // BLENDS_G
    tile_index = (group_of[:, None] * TILES_G + blend_source * TILE_DEV + blend_slot).astype(jnp.int32)
    blocks = BLENDS_ALL // BLEND_DEV

    def visit(summed, inputs):
        rows, sed, morph, count = inputs
        blend_data = pixel_tiles[rows].astype(jnp.bfloat16)
        sed_new, model_out = fit_block(blend_data, sed, morph, count)
        summed = summed.at[rows.reshape(-1)].add(model_out.reshape(-1, BANDS, PIX).astype(jnp.float32))
        return (summed, sed_new)
    summed, sed_blocks = lax.scan(visit, jnp.zeros((TILES_ALL, BANDS, PIX), jnp.float32), (tile_index.reshape(blocks, BLEND_DEV, FOOT), sed_start.reshape(blocks, BLEND_DEV, COMPONENTS, BANDS), morph_start.reshape(blocks, BLEND_DEV, FOOT, COMPONENTS, PIX), component_count.reshape(blocks, BLEND_DEV)))
    residual = pixel_tiles - summed
    total_sq = jnp.sum(residual * residual)
    whitened = residual / jnp.sqrt(total_sq / float(TILES_ALL * BANDS * PIX) + 1e-06)
    return (whitened, sed_blocks.reshape(BLENDS_ALL, COMPONENTS, BANDS))
```

```python
import functools
import math

import jax
import jax.numpy as jnp
from jax import lax
from jax.experimental import pallas as pl
from jax.experimental.pallas import tpu as pltpu
from jax.sharding import PartitionSpec as P

ITERS = 2
CHUNKS = 2
F32 = jnp.float32
BF16 = jnp.bfloat16
MESH = pl.DeviceIdType.MESH


def dot(a, b):
    return jnp.dot(a, b, preferred_element_type=F32)


def dot_nt(a, b):
    return lax.dot_general(a, b, (((1,), (1,)), ((), ())), preferred_element_type=F32)


def iota(shape, dimension):
    return lax.broadcasted_iota(jnp.int32, shape, dimension)


def split_row(shape, dimension, width):
    place = iota(shape, dimension)
    out = jnp.zeros(shape, jnp.int32)
    for cut in range(width, shape[dimension], width):
        out = out + (place >= cut).astype(jnp.int32)
    return out, place - out * width


def kernel(
    peers, regions, stride, size, tiles, source, slot, count, sed0, morph_hbm, white, sed_out,
    morph_in, mor, tgt, gram, seds, mod, pt, ptt, req, wanted, send, arrived, outb, ret, part, parts,
    in_sem, ask_s, ask_r, put_s, put_r, back_s, back_r, sum_s, sum_r,
):
    bands, tile_rows, pixels = tiles.shape
    foot, rows = source.shape
    comps = sed0.shape[1]
    groups = rows // size
    slots = peers * stride
    me = lax.axis_index("dev")
    everyone = peers * regions
    my = lax.axis_index("grp") * peers + me
    load = pltpu.make_async_copy(morph_hbm, morph_in, in_sem)
    load.start()
    barrier = pltpu.get_barrier_semaphore()

    def greet(step, carry):
        other = lax.rem(my + step, everyone)
        pl.semaphore_signal(
            barrier, inc=1, device_id={"grp": other // peers, "dev": lax.rem(other, peers)},
            device_id_type=MESH,
        )
        return carry

    lax.fori_loop(1, everyone, greet, 0)

    upper = (iota((rows, rows), 0) <= iota((rows, rows), 1)).astype(F32).astype(BF16)
    base = jnp.zeros((peers, 1), F32)
    want = jnp.zeros((slots, 1), F32)
    for f in range(foot):
        named = source[f : f + 1, :]
        hit = (iota((peers, rows), 0) == named).astype(F32)
        seen = dot(hit.astype(BF16), upper) + base
        rank = jnp.sum(hit * (seen - 1.0), axis=0, keepdims=True)
        base = base + jnp.sum(hit, axis=1, keepdims=True)
        place = named.astype(F32) * float(stride) + rank
        put = (iota((slots, rows), 0).astype(F32) == place).astype(F32)
        pt[f] = put.astype(BF16)
        ptt[f] = jnp.transpose(put).astype(BF16)
        want = want + jnp.sum(put * (slot[f : f + 1, :].astype(F32) + 1.0), axis=1, keepdims=True)
    req[...] = (
        jnp.broadcast_to(want, (slots, 128)).astype(jnp.int32).reshape(peers, stride, 128)
    )
    pl.semaphore_wait(barrier, everyone - 1)

    def exchange(src, dst, send_sem, recv_sem, lanes=None, at=None):
        def part_of(ref, index):
            return ref.at[index] if lanes is None else ref.at[index, :, lanes]

        def sem(ref, step):
            return ref.at[step] if at is None else ref.at[at, step]

        def copy(step, incoming):
            there = lax.rem(me + step, peers)
            here = lax.rem(me - step + peers, peers) if incoming else me
            return pltpu.make_async_remote_copy(
                src_ref=part_of(src, there), dst_ref=part_of(dst, here),
                send_sem=sem(send_sem, step), recv_sem=sem(recv_sem, step),
                device_id={"dev": there}, device_id_type=MESH,
            )

        def start():
            def body(step, carry):
                copy(step, False).start()
                return carry

            lax.fori_loop(1, peers, body, 0)

        def wait_in():
            def body(step, carry):
                copy(step, True).wait_recv()
                return carry

            lax.fori_loop(1, peers, body, 0)

        def wait_out():
            def body(step, carry):
                copy(step, False).wait_send()
                return carry

            lax.fori_loop(1, peers, body, 0)

        return start, wait_in, wait_out

    ask, ask_in, ask_out = exchange(req, wanted, ask_s, ask_r)
    ask()
    wanted[me] = req[me]

    width = size * comps
    span = size * bands
    blend_row, comp_row = split_row((width, 1), 0, comps)
    blend_col, _ = split_row((1, width), 1, comps)
    band_col, member_col = split_row((1, span), 1, size)
    same = (blend_row == blend_col).astype(F32)
    same_bd = (blend_row == member_col).astype(F32)
    spread = (iota((width, comps), 1) == comp_row).astype(F32).astype(BF16)
    gather_k = (
        iota((comps, width), 0) == split_row((1, width), 1, comps)[1]
    ).astype(F32).astype(BF16)
    sed_all = jnp.concatenate([sed0[b].astype(F32) for b in range(bands)], axis=1).astype(BF16)
    band_of, blend_of = split_row((bands * rows, 1), 0, rows)

    def chosen(g):
        return (
            ((band_of == band_col) & (blend_of == g * size + member_col)).astype(F32)
        )

    load.wait()

    def begin(g, carry):
        held = jnp.sum(
            jnp.where(iota((width, rows), 1) == g * size + blend_row, count[...], 0).astype(F32),
            axis=1, keepdims=True,
        )
        active = (comp_row.astype(F32) < held).astype(F32)
        first = dot(sed_all, chosen(g).astype(BF16))
        seds[g] = dot(spread, first.astype(BF16)) * same_bd * active
        total = jnp.zeros((width, width), F32)
        for f in range(foot):
            whole = morph_in[pl.ds(g * size, size), f].astype(F32).reshape(width, pixels)
            masked = (whole * active).astype(BF16)
            mor[g, f] = masked
        return carry

    lax.fori_loop(0, groups, begin, 0)
    ask_in()
    picks = (wanted[...].reshape(slots, 128)[:, :tile_rows] - 1 == iota((slots, tile_rows), 1)).astype(F32)
    pick = picks.astype(BF16)
    for b in range(bands):
        block = dot(pick, tiles[b].astype(BF16)).astype(BF16).astype(F32)
        send[:, :, b * pixels : (b + 1) * pixels] = block.reshape(peers, stride, pixels).astype(BF16)
    fetch, fetch_in, fetch_out = exchange(send, arrived, put_s, put_r)
    fetch()
    arrived[me] = send[me]

    def first_gram(g, carry):
        total = dot_nt(mor[g, 0], mor[g, 0])
        for f in range(1, foot):
            total = total + dot_nt(mor[g, f], mor[g, f])
        gram[g] = total * same
        return carry

    lax.fori_loop(0, groups, first_gram, 0)
    fetch_in()
    for b in range(bands):
        block = arrived[:, :, b * pixels : (b + 1) * pixels].astype(F32)
        block = block.reshape(slots, pixels).astype(BF16)
        for f in range(foot):
            tgt[:, f, b * size : (b + 1) * size, :] = dot(ptt[f], block).reshape(
                groups, size, pixels
            )

    def norm(square, mask):
        flat = jnp.sum(square, axis=0, keepdims=True)
        return jnp.sqrt(jnp.sum(mask * flat, axis=1, keepdims=True)) + 1.0

    def fit(g, placed):
        sed = seds[g]
        for sweep in range(ITERS):
            if sweep == 0:
                grams = gram[g]
            else:
                grams = dot_nt(mor[g, 0], mor[g, 0])
                for f in range(1, foot):
                    grams = grams + dot_nt(mor[g, f], mor[g, f])
                grams = grams * same
            cross = dot_nt(mor[g, 0], tgt[g, 0].astype(BF16))
            for f in range(1, foot):
                cross = cross + dot_nt(mor[g, f], tgt[g, f].astype(BF16))
            step = 1.0 / norm(grams * grams, same)
            slope = dot(grams.astype(BF16), sed.astype(BF16)) - cross * same_bd
            sed = jnp.maximum(sed - slope * step, 0.0).astype(BF16).astype(F32)
            sed_b = sed.astype(BF16)
            sed_t = jnp.transpose(sed).astype(BF16)
            small = dot(sed_t, sed_b)
            step = 1.0 / norm(small * small, same_bd)
            for f in range(foot):
                misfit = (dot(sed_t, mor[g, f]) - tgt[g, f]).astype(BF16)
                slope = dot(sed_b, misfit)
                mor[g, f] = jnp.maximum(
                    mor[g, f].astype(F32) - (slope + 0.1) * step, 0.0
                ).astype(BF16)
        for f in range(foot):
            mod[f, :, pl.ds(pl.multiple_of(g * size, size), size), :] = dot(
                sed_t, mor[g, f]
            ).reshape(bands, size, pixels)
        lean = dot(gather_k, sed_b)
        return placed + dot_nt(lean.astype(BF16), chosen(g).astype(BF16))

    placed = lax.fori_loop(0, groups, fit, jnp.zeros((comps, bands * rows), F32))
    for b in range(bands):
        sed_out[b] = placed[:, b * rows : (b + 1) * rows].astype(BF16)

    each = bands // CHUNKS
    trips = []
    for chunk in range(CHUNKS):
        for b in range(chunk * each, (chunk + 1) * each):
            block = dot(pt[0], mod[0, b].astype(BF16))
            for f in range(1, foot):
                block = block + dot(pt[f], mod[f, b].astype(BF16))
            outb[:, :, b * pixels : (b + 1) * pixels] = block.reshape(
                peers, stride, pixels
            ).astype(BF16)
        lanes = slice(chunk * each * pixels, (chunk + 1) * each * pixels)
        trips.append(exchange(outb, ret, back_s, back_r, lanes, chunk))
        trips[-1][0]()
    ret[me] = outb[me]
    pick_t = jnp.transpose(picks).astype(BF16)
    squares = jnp.zeros((8, 128), F32)
    for chunk in range(CHUNKS):
        trips[chunk][1]()
        for b in range(chunk * each, (chunk + 1) * each):
            block = ret[:, :, b * pixels : (b + 1) * pixels].astype(F32)
            block = block.reshape(slots, pixels).astype(BF16)
            residual = tiles[b] - dot(pick_t, block)
            white[b] = residual
            square = residual * residual
            for r in range(0, tile_rows, 8):
                for c in range(0, pixels, 128):
                    squares = squares + square[r : r + 8, c : c + 128]

    part[...] = squares

    def share(step, incoming):
        there = lax.rem(my + step, everyone)
        here = lax.rem(my - step + everyone, everyone) if incoming else my
        return pltpu.make_async_remote_copy(
            src_ref=part, dst_ref=parts.at[here], send_sem=sum_s.at[step],
            recv_sem=sum_r.at[step],
            device_id={"grp": there // peers, "dev": lax.rem(there, peers)}, device_id_type=MESH,
        )

    def start_share(step, carry):
        share(step, False).start()
        return carry

    def end_share(step, carry):
        share(step, True).wait_recv()
        return carry

    def end_sent(step, carry):
        share(step, False).wait_send()
        return carry

    lax.fori_loop(1, everyone, start_share, 0)
    parts[my] = squares
    ask_out()
    fetch_out()
    for trip in trips:
        trip[2]()
    lax.fori_loop(1, everyone, end_share, 0)
    total = jnp.sum(parts[...], axis=0)
    total = jnp.sum(jnp.sum(total, axis=1, keepdims=True), axis=0, keepdims=True)
    count_all = float(bands * tile_rows * pixels * everyone)
    scale = 1.0 / jnp.sqrt(total / count_all + 1e-06)
    for b in range(bands):
        white[b] = white[b] * scale
    lax.fori_loop(1, everyone, end_sent, 0)


def on_device(pixel_tiles, blend_source, blend_slot, component_count, sed_start, morph_start):
    peers = lax.axis_size("dev")
    regions = lax.axis_size("grp")
    rows, foot = blend_source.shape
    tile_rows, bands, pixels = pixel_tiles.shape
    comps = sed_start.shape[1]
    entries = rows * foot
    capacity = max(2, (entries + peers - 1) // peers)
    stride = (capacity + 7) // 8 * 8
    size = math.gcd(rows, 8)
    groups = rows // size
    slots = peers * stride
    flat = bands * pixels
    vmem = pl.BlockSpec(memory_space=pltpu.VMEM)
    dma = pltpu.SemaphoreType.DMA
    white, sed_final = pl.pallas_call(
        functools.partial(kernel, peers, regions, stride, size),
        out_shape=(
            jax.ShapeDtypeStruct((bands, tile_rows, pixels), F32),
            jax.ShapeDtypeStruct((bands, comps, rows), BF16),
        ),
        in_specs=[vmem] * 5 + [pl.BlockSpec(memory_space=pl.ANY)],
        out_specs=(vmem, vmem),
        scratch_shapes=[
            pltpu.VMEM(morph_start.shape, BF16),
            pltpu.VMEM((groups, foot, size * comps, pixels), BF16),
            pltpu.VMEM((groups, foot, size * bands, pixels), F32),
            pltpu.VMEM((groups, size * comps, size * comps), F32),
            pltpu.VMEM((groups, size * comps, size * bands), F32),
            pltpu.VMEM((foot, bands, rows, pixels), F32),
            pltpu.VMEM((foot, slots, rows), BF16),
            pltpu.VMEM((foot, rows, slots), BF16),
            pltpu.VMEM((peers, stride, 128), jnp.int32),
            pltpu.VMEM((peers, stride, 128), jnp.int32),
            pltpu.VMEM((peers, stride, flat), BF16),
            pltpu.VMEM((peers, stride, flat), BF16),
            pltpu.VMEM((peers, stride, flat), BF16),
            pltpu.VMEM((peers, stride, flat), BF16),
            pltpu.VMEM((8, 128), F32),
            pltpu.VMEM((peers * regions, 8, 128), F32),
            dma,
            dma((peers,)),
            dma((peers,)),
            dma((peers,)),
            dma((peers,)),
            dma((CHUNKS, peers)),
            dma((CHUNKS, peers)),
            dma((peers * regions,)),
            dma((peers * regions,)),
        ],
        compiler_params=pltpu.CompilerParams(
            collective_id=0, has_side_effects=True, vmem_limit_bytes=60 * 1024 * 1024
        ),
    )(
        jnp.transpose(pixel_tiles, (1, 0, 2)),
        jnp.transpose(blend_source),
        jnp.transpose(blend_slot),
        component_count.reshape(1, rows),
        jnp.transpose(sed_start, (2, 1, 0)),
        morph_start,
    )
    return jnp.transpose(white, (1, 0, 2)), jnp.transpose(sed_final, (2, 1, 0))


def solution(mesh):
    placed = (
        P(("grp", "dev"), None, None),
        P(("grp", "dev"), None),
        P(("grp", "dev"), None),
        P(("grp", "dev")),
        P(("grp", "dev"), None, None),
        P(("grp", "dev"), None, None, None),
    )
    return jax.shard_map(
        on_device,
        mesh=mesh,
        in_specs=placed,
        out_specs=(P(("grp", "dev"), None, None), P(("grp", "dev"), None, None)),
        check_vma=False,
    )
```

```python
import functools
import math

import jax
import jax.numpy as jnp
from jax import lax
from jax.experimental import pallas as pl
from jax.experimental.pallas import tpu as pltpu
from jax.sharding import PartitionSpec as P

INWARD = 1
OUTWARD = 2
F32 = jnp.float32
BF16 = jnp.bfloat16
MESH = pl.DeviceIdType.MESH


def dot(a, b):
    return jnp.dot(a, b, preferred_element_type=F32)


def dot_nt(a, b):
    return lax.dot_general(a, b, (((1,), (1,)), ((), ())), preferred_element_type=F32)


def iota(shape, dimension):
    return lax.broadcasted_iota(jnp.int32, shape, dimension)


def split_row(shape, dimension, width):
    place = iota(shape, dimension)
    out = jnp.zeros(shape, jnp.int32)
    for cut in range(width, shape[dimension], width):
        out = out + (place >= cut).astype(jnp.int32)
    return out, place - out * width


def kernel(
    peers, regions, stride, size, tiles, source, slot, count, sed0, morph_hbm, white, sed_out, scale_out,
    morph_in, mor, tgt, mis, gram, seds, sed_b, sed_step, morph_step, mod, pt, ptt, req, wanted, send, arrived, outb, ret, part, parts,
    in_sem, ask_s, ask_r, put_s, put_r, back_s, back_r, sum_s, sum_r,
):
    bands, tile_rows, pixels = tiles.shape
    foot, rows = source.shape
    comps = sed0.shape[1]
    groups = rows // size
    slots = peers * stride
    me = lax.axis_index("dev")
    everyone = peers * regions
    my = lax.axis_index("grp") * peers + me
    load = pltpu.make_async_copy(morph_hbm, morph_in, in_sem)
    load.start()
    barrier = pltpu.get_barrier_semaphore()

    def greet(step, carry):
        other = lax.rem(my + step, everyone)
        pl.semaphore_signal(
            barrier, inc=1, device_id={"grp": lax.div(other, peers), "dev": lax.rem(other, peers)},
            device_id_type=MESH,
        )
        return carry

    lax.fori_loop(1, everyone, greet, 0)

    upper = (iota((rows, rows), 0) <= iota((rows, rows), 1)).astype(F32).astype(BF16)
    base = jnp.zeros((peers, 1), F32)
    want = jnp.zeros((slots, 1), F32)
    for f in range(foot):
        named = source[f : f + 1, :]
        hit = (iota((peers, rows), 0) == named).astype(F32)
        seen = dot(hit.astype(BF16), upper) + base
        rank = jnp.sum(hit * (seen - 1.0), axis=0, keepdims=True)
        base = base + jnp.sum(hit, axis=1, keepdims=True)
        place = named.astype(F32) * float(stride) + rank
        put = (iota((slots, rows), 0).astype(F32) == place).astype(F32)
        pt[f] = put.astype(BF16)
        ptt[f] = jnp.transpose(put).astype(BF16)
        want = want + jnp.sum(put * (slot[f : f + 1, :].astype(F32) + 1.0), axis=1, keepdims=True)
    req[...] = (
        jnp.broadcast_to(want, (slots, 128)).astype(jnp.int32).reshape(peers, stride, 128)
    )
    pl.semaphore_wait(barrier, everyone - 1)

    def exchange(src, dst, send_sem, recv_sem, lanes=None, at=None):
        def part_of(ref, index):
            return ref.at[index] if lanes is None else ref.at[index, :, lanes]

        def sem(ref, step):
            return ref.at[step] if at is None else ref.at[at, step]

        def copy(step, incoming):
            there = lax.rem(me + step, peers)
            here = lax.rem(me - step + peers, peers) if incoming else me
            return pltpu.make_async_remote_copy(
                src_ref=part_of(src, there), dst_ref=part_of(dst, here),
                send_sem=sem(send_sem, step), recv_sem=sem(recv_sem, step),
                device_id={"dev": there}, device_id_type=MESH,
            )

        def start():
            def body(step, carry):
                copy(step, False).start()
                return carry

            lax.fori_loop(1, peers, body, 0)

        def wait_in():
            def body(step, carry):
                copy(step, True).wait_recv()
                return carry

            lax.fori_loop(1, peers, body, 0)

        def wait_out():
            def body(step, carry):
                copy(step, False).wait_send()
                return carry

            lax.fori_loop(1, peers, body, 0)

        return start, wait_in, wait_out

    ask, ask_in, ask_out = exchange(req, wanted, ask_s, ask_r)
    ask()
    wanted[me] = req[me]

    width = size * comps
    span = size * bands
    blend_row, comp_row = split_row((width, 1), 0, comps)
    blend_col, comp_col = split_row((1, width), 1, comps)
    _, member_col = split_row((1, span), 1, size)
    band_row, member_row = split_row((span, 1), 0, size)
    same = (blend_row == blend_col).astype(F32)
    same_bd = (blend_row == member_col).astype(F32)
    same_t = (member_row == blend_col).astype(F32)
    gather_k = (iota((comps, width), 0) == comp_col).astype(F32).astype(BF16)
    sed_all = jnp.concatenate([sed0[b].astype(F32) for b in range(bands)], axis=1).astype(BF16)
    band_of, blend_of = split_row((1, bands * rows), 1, rows)
    counts = jnp.broadcast_to(count[...], (8, rows)).astype(F32).astype(BF16)
    pair = 2 if groups % 2 == 0 else 1

    def chosen(g):
        hit = (band_of == band_row) & (blend_of == g * size + member_row)
        return hit.astype(F32).astype(BF16)

    def norm(square, mask):
        flat = jnp.sum(square, axis=0, keepdims=True)
        return jnp.sqrt(jnp.sum(mask * flat, axis=1, keepdims=True)) + 1.0

    def wide(column):
        return jnp.broadcast_to(column, (column.shape[0], 128))

    def over_groups(body, pair=pair):
        def both(j, carry):
            stores = []
            for k in range(pair):
                stores = stores + body(j * pair + k)
            for ref, index, value in stores:
                ref[index] = value
            return carry

        lax.fori_loop(0, groups // pair, both, 0)

    load.wait()

    def begin(g):
        held = jnp.sum(
            jnp.where(iota((width, rows), 1) == g * size + blend_row, count[...], 0).astype(F32),
            axis=1, keepdims=True,
        )
        active = (comp_row.astype(F32) < held).astype(F32)
        owner = (iota((rows, width), 0) == g * size + blend_col).astype(F32).astype(BF16)
        active_t = (comp_col.astype(F32) < dot(counts, owner)[0:1]).astype(F32)
        first = dot_nt(chosen(g), sed_all)
        stores = [(seds, g, dot(first.astype(BF16), gather_k) * same_t * active_t)]
        for f in range(foot):
            whole = morph_in[pl.ds(g * size, size), f].astype(F32).reshape(width, pixels)
            stores.append((mor, (g, f), (whole * active).astype(BF16)))
        return stores

    over_groups(begin)
    ask_in()
    picks = (wanted[...].reshape(slots, 128)[:, :tile_rows] - 1 == iota((slots, tile_rows), 1)).astype(F32)
    pick = picks.astype(BF16)
    arrivals = INWARD if bands % INWARD == 0 else 1
    each = bands // arrivals
    fetches = []
    for c in range(arrivals):
        for b in range(c * each, (c + 1) * each):
            block = dot(pick, tiles[b].astype(BF16))
            send[:, :, b * pixels : (b + 1) * pixels] = block.reshape(
                peers, stride, pixels
            ).astype(BF16)
        lanes = slice(c * each * pixels, (c + 1) * each * pixels)
        fetches.append(exchange(send, arrived, put_s, put_r, lanes, c))
        fetches[-1][0]()
    arrived[me] = send[me]

    def grams_of(morphs):
        total = dot_nt(morphs[0], morphs[0])
        for f in range(1, foot):
            total = total + dot_nt(morphs[f], morphs[f])
        return total * same

    def cross_of(targets, morphs):
        total = dot_nt(targets[0], morphs[0])
        for f in range(1, foot):
            total = total + dot_nt(targets[f], morphs[f])
        return total

    def first_gram(g):
        total = grams_of([mor[g, f] for f in range(foot)])
        step = 1.0 / norm(total * total, same_t)
        return [(gram, g, total.astype(BF16)), (sed_step, g, wide(step))]

    over_groups(first_gram)

    for c in range(arrivals):
        fetches[c][1]()
        for b in range(c * each, (c + 1) * each):
            block = arrived[:, :, b * pixels : (b + 1) * pixels].astype(F32)
            block = block.reshape(slots, pixels).astype(BF16)
            for f in range(foot):
                tgt[:, f, b * size : (b + 1) * size, :] = dot(ptt[f], block).reshape(
                    groups, size, pixels
                )
        part_rows = slice(c * each * size, (c + 1) * each * size)

        def first_seds(g):
            targets = [tgt[g, f, part_rows] for f in range(foot)]
            morphs = [mor[g, f] for f in range(foot)]
            cross = cross_of([t.astype(BF16) for t in targets], morphs) * same_t[part_rows]
            old = seds[g, part_rows]
            slope = dot(old.astype(BF16), gram[g]) - cross
            sed = jnp.maximum(old - slope * sed_step[g, part_rows, 0:1], 0.0).astype(BF16)
            stores = [(seds, (g, part_rows), sed.astype(F32))]
            for f in range(foot):
                misfit = (dot(sed, morphs[f]) - targets[f]).astype(BF16)
                stores.append((mis, (g, f, part_rows), misfit))
            return stores

        over_groups(first_seds)

    def moved(morph, slope, step):
        return jnp.maximum(morph.astype(F32) - (slope + 0.1) * step, 0.0).astype(BF16)

    def morph_stepsize(sed):
        small = dot_nt(sed, sed)
        return 1.0 / norm(small * small, same_bd)

    def second_seds(g):
        old = seds[g]
        step = morph_stepsize(old.astype(BF16))
        lhs = jnp.transpose(old).astype(BF16)
        morphs = [moved(mor[g, f], dot(lhs, mis[g, f]), step) for f in range(foot)]
        stores = [(mor, (g, f), morphs[f]) for f in range(foot)]
        total = grams_of(morphs)
        cross = cross_of([tgt[g, f].astype(BF16) for f in range(foot)], morphs) * same_t
        slope = dot(old.astype(BF16), total.astype(BF16)) - cross
        sed = jnp.maximum(old - slope / norm(total * total, same_t), 0.0).astype(BF16)
        stores.append((seds, g, sed.astype(F32)))
        stores.append((sed_b, g, jnp.transpose(sed.astype(F32)).astype(BF16)))
        stores.append((morph_step, g, wide(morph_stepsize(sed))))
        return stores

    over_groups(second_seds)

    window = pixels // OUTWARD
    trips = []
    for chunk in range(OUTWARD):
        taken = slice(chunk * window, (chunk + 1) * window)

        def last_models(g):
            sed = seds[g].astype(BF16)
            stores = []
            for f in range(foot):
                morph = mor[g, f, :, taken]
                misfit = (dot(sed, morph) - tgt[g, f, :, taken]).astype(BF16)
                morph = moved(morph, dot(sed_b[g], misfit), morph_step[g, :, 0:1])
                model = dot(sed, morph).reshape(bands, size, window)
                member = pl.ds(pl.multiple_of(g * size, size), size)
                stores.append((mod, (f, slice(None), member, slice(None)), model))
            return stores

        over_groups(last_models)
        for b in range(bands):
            block = dot(pt[0], mod[0, b].astype(BF16))
            for f in range(1, foot):
                block = block + dot(pt[f], mod[f, b].astype(BF16))
            at = (chunk * bands + b) * window
            outb[:, :, at : at + window] = block.reshape(peers, stride, window).astype(BF16)
        lanes = slice(chunk * bands * window, (chunk + 1) * bands * window)
        trips.append(exchange(outb, ret, back_s, back_r, lanes, chunk))
        trips[-1][0]()
    ret[me] = outb[me]

    def place(g, placed):
        lean = dot_nt(gather_k, seds[g].astype(BF16))
        return placed + dot(lean.astype(BF16), chosen(g))

    placed = lax.fori_loop(0, groups, place, jnp.zeros((comps, bands * rows), F32))
    for b in range(bands):
        sed_out[b] = placed[:, b * rows : (b + 1) * rows].astype(BF16)
    pick_t = jnp.transpose(picks).astype(BF16)
    squares = jnp.zeros((8, 128), F32)
    for chunk in range(OUTWARD):
        trips[chunk][1]()
        taken = slice(chunk * window, (chunk + 1) * window)
        for b in range(bands):
            at = (chunk * bands + b) * window
            block = ret[:, :, at : at + window].astype(F32).reshape(slots, window).astype(BF16)
            residual = tiles[b, :, taken] - dot(pick_t, block)
            white[b, :, taken] = residual
            square = residual * residual
            for r in range(0, tile_rows, 8):
                for c in range(0, window, 128):
                    squares = squares + square[r : r + 8, c : c + 128]

    own_row = jnp.sum(squares, axis=0, keepdims=True)
    part[...] = own_row

    def share(step, incoming):
        there = lax.rem(my + step, everyone)
        here = lax.rem(my - step + everyone, everyone) if incoming else my
        return pltpu.make_async_remote_copy(
            src_ref=part, dst_ref=parts.at[here], send_sem=sum_s.at[step],
            recv_sem=sum_r.at[step],
            device_id={"grp": lax.div(there, peers), "dev": lax.rem(there, peers)}, device_id_type=MESH,
        )

    def start_share(step, carry):
        share(step, False).start()
        return carry

    def end_share(step, carry):
        share(step, True).wait_recv()
        return carry

    def end_sent(step, carry):
        share(step, False).wait_send()
        return carry

    lax.fori_loop(1, everyone, start_share, 0)
    parts[my] = own_row
    ask_out()
    for trip in fetches + trips:
        trip[2]()
    lax.fori_loop(1, everyone, end_share, 0)
    total = jnp.sum(parts[...], axis=0)
    total = jnp.sum(jnp.sum(total, axis=1, keepdims=True), axis=0, keepdims=True)
    count_all = float(bands * tile_rows * pixels * everyone)
    scale_out[...] = jnp.broadcast_to(1.0 / jnp.sqrt(total / count_all + 1e-06), (8, 128))
    lax.fori_loop(1, everyone, end_sent, 0)


def on_device(pixel_tiles, blend_source, blend_slot, component_count, sed_start, morph_start):
    peers = lax.axis_size("dev")
    regions = lax.axis_size("grp")
    rows, foot = blend_source.shape
    tile_rows, bands, pixels = pixel_tiles.shape
    comps = sed_start.shape[1]
    entries = rows * foot
    capacity = max(2, (entries + peers - 1) // peers)
    stride = (capacity + 7) // 8 * 8
    size = math.gcd(rows, 8)
    groups = rows // size
    slots = peers * stride
    flat = bands * pixels
    vmem = pl.BlockSpec(memory_space=pltpu.VMEM)
    dma = pltpu.SemaphoreType.DMA
    residual, sed_final, scale = pl.pallas_call(
        functools.partial(kernel, peers, regions, stride, size),
        out_shape=(
            jax.ShapeDtypeStruct((bands, tile_rows, pixels), F32),
            jax.ShapeDtypeStruct((bands, comps, rows), BF16),
            jax.ShapeDtypeStruct((8, 128), F32),
        ),
        in_specs=[vmem] * 5 + [pl.BlockSpec(memory_space=pl.ANY)],
        out_specs=(vmem, vmem, vmem),
        scratch_shapes=[
            pltpu.VMEM(morph_start.shape, BF16),
            pltpu.VMEM((groups, foot, size * comps, pixels), BF16),
            pltpu.VMEM((groups, foot, size * bands, pixels), F32),
            pltpu.VMEM((groups, foot, size * bands, pixels), BF16),
            pltpu.VMEM((groups, size * comps, size * comps), BF16),
            pltpu.VMEM((groups, size * bands, size * comps), F32),
            pltpu.VMEM((groups, size * comps, size * bands), BF16),
            pltpu.VMEM((groups, size * bands, 128), F32),
            pltpu.VMEM((groups, size * comps, 128), F32),
            pltpu.VMEM((foot, bands, rows, pixels // OUTWARD), F32),
            pltpu.VMEM((foot, slots, rows), BF16),
            pltpu.VMEM((foot, rows, slots), BF16),
            pltpu.VMEM((peers, stride, 128), jnp.int32),
            pltpu.VMEM((peers, stride, 128), jnp.int32),
            pltpu.VMEM((peers, stride, flat), BF16),
            pltpu.VMEM((peers, stride, flat), BF16),
            pltpu.VMEM((peers, stride, flat), BF16),
            pltpu.VMEM((peers, stride, flat), BF16),
            pltpu.VMEM((1, 128), F32),
            pltpu.VMEM((peers * regions, 1, 128), F32),
            dma,
            dma((peers,)),
            dma((peers,)),
            dma((INWARD, peers)),
            dma((INWARD, peers)),
            dma((OUTWARD, peers)),
            dma((OUTWARD, peers)),
            dma((peers * regions,)),
            dma((peers * regions,)),
        ],
        compiler_params=pltpu.CompilerParams(
            collective_id=0, has_side_effects=True, vmem_limit_bytes=60 * 1024 * 1024
        ),
    )(
        jnp.transpose(pixel_tiles, (1, 0, 2)),
        jnp.transpose(blend_source),
        jnp.transpose(blend_slot),
        component_count.reshape(1, rows),
        jnp.transpose(sed_start, (2, 1, 0)),
        morph_start,
    )
    white = residual * scale[0, 0]
    return jnp.transpose(white, (1, 0, 2)), jnp.transpose(sed_final, (2, 1, 0))


def solution(mesh):
    placed = (
        P(("grp", "dev"), None, None),
        P(("grp", "dev"), None),
        P(("grp", "dev"), None),
        P(("grp", "dev")),
        P(("grp", "dev"), None, None),
        P(("grp", "dev"), None, None, None),
    )
    return jax.shard_map(
        on_device,
        mesh=mesh,
        in_specs=placed,
        out_specs=(P(("grp", "dev"), None, None), P(("grp", "dev"), None, None)),
        check_vma=False,
    )
```
